512 devices in a mesh: gx: 8 (over z), gy: 4 (over x), gz: 16 (over y, core).
Axes of the slice: x: 4, y: 8, z: 8, core: 2. Of those that a mesh axis runs over, the one named last changes fastest.
Arguments:
- acts: bfloat16 [655360, 768], P(('gx', 'gy', 'gz')), may hold values from -24 to 24
- grads_out: bfloat16 [655360, 768], P(('gx', 'gy', 'gz')), may hold values from -0.0078125 to 0.0078125
- master: float32 [4608, 128], P(('gx', 'gy', 'gz')), may hold values from -0.3 to 0.3
- moment: float32 [4608, 128], P(('gx', 'gy', 'gz')), may hold values from -6 to 6
- second: float32 [4608, 128], P(('gx', 'gy', 'gz')), may hold values from 0.1 to 2
Outputs:
- master_new: float32 [4608, 128], P(('gx', 'gy', 'gz'))
- moment_new: float32 [4608, 128], P(('gx', 'gy', 'gz'))
- second_new: float32 [4608, 128], P(('gx', 'gy', 'gz'))
- weights: bfloat16 [768, 768], replicated
The draws below stay inside these ranges and needn't reach their ends.
All inputs are finite; a program needn't handle non-finite values.
Results may differ from the reference program's by a relative error of at most 0.003.
Values may be sent and summed in bfloat16 or wider, within the bound.
A program may use at most 64 MiB of HBM per device.

```python
import math
import jax
import jax.numpy as jnp
from jax import lax

IN = 768
OUT = 768
LANE = 128
STEP = 1000
TOK_DEV = 1280
TOKENS = 655360
FLAT = 4608


def spiked(result, own_key, source, target, shards_of, factor):
    def block_of(position):
        return (jnp.arange(result.shape[position]) // (result.shape[position] // shards_of)).reshape((-1,) + (1,) * (result.ndim - 1 - position))

    one_side = jax.random.permutation(own_key, shards_of)[block_of(target)]
    far = (block_of(target) + shards_of // 2) % shards_of
    return jnp.where((block_of(source) == one_side) | (block_of(source) == far), factor * result, result)


def block_levels(key, extent, cuts, least, top_value):
    gain, own = 1.0, jax.random.fold_in(key, 6)
    for dim, blocks in cuts:
        steps = jnp.exp(jax.random.uniform(jax.random.fold_in(own, dim), (blocks,), jnp.float32, least / len(cuts), top_value / len(cuts)))
        gain = gain * jnp.repeat(steps, extent[dim] // blocks).reshape([-1 if axis == dim else 1 for axis in range(len(extent))])
    return gain


def noise(own_key, shape, width, reach, shards=(), held_as=jnp.bfloat16):
    drawn = jax.random.normal(own_key, shape, jnp.float32) * width
    if len(shards) > 0:
        drawn = block_levels(own_key, shape, shards, -0.22, 0.18) * drawn
    return jnp.clip(drawn, min=-reach, max=reach).astype(held_as)


def gaussian_with(rng, shape, spread, reach, pieces, heavy, kind=jnp.bfloat16):
    array = spread * jax.random.normal(rng, shape, jnp.float32)
    if pieces:
        array = array * block_levels(rng, shape, pieces, -0.22, 0.18)
    return jnp.clip(spiked(array, jax.random.fold_in(rng, 3), *heavy), -reach, reach).astype(kind)


def setup_inputs(seed: int = 0) -> dict:
    keys = jax.random.split(jax.random.key(seed), 6)
    return {
        "acts": gaussian_with(keys[0], (TOKENS, IN), 1.0, 24.0, ((0, 512),), (0, 1, 256, 6.0)),
        "grads_out": noise(keys[1], (TOKENS, OUT), TOKENS ** -0.5, 0.0078125, ((0, 512),)),
        "master": noise(keys[2], (FLAT, LANE), 0.05, 0.3, ((0, 512),), jnp.float32),
        "moment": noise(keys[3], (FLAT, LANE), 1.0, 6.0, ((0, 512),), jnp.float32),
        "second": jnp.clip(jnp.exp(math.log(2.0) - 2.9957323 * jax.random.uniform(keys[4], (FLAT, LANE), jnp.float32) ** block_levels(keys[4], (FLAT, LANE), ((0, 512),), -0.2, 0.2)), 0.1, 2.0),
    }


def reference(acts, grads_out, master, moment, second):
    blocks = TOKENS // TOK_DEV
    act_blocks = acts.reshape(blocks, TOK_DEV, IN)
    cot_blocks = grads_out.reshape(blocks, TOK_DEV, OUT)

    def add_block(total, pair):
        product = lax.dot_general(pair[0], pair[1], (((0,), (0,)), ((), ())), preferred_element_type=jnp.float32)
        return (total + product, None)
    start = jnp.zeros((IN, OUT), jnp.float32)
    gradient, _ = lax.scan(add_block, start, (act_blocks, cot_blocks))
    gradient = gradient.reshape(FLAT, LANE)
    moment_new = 0.9 * moment + 0.1 * gradient
    second_new = 0.95 * second + 0.05 * gradient * gradient
    first_fix = 1.0 - 0.9 ** STEP
    second_fix = 1.0 - 0.95 ** STEP
    ratio = moment_new / first_fix / (jnp.sqrt(second_new / second_fix) + 1e-08)
    master_new = master - 0.01 * (ratio + 0.01 * master)
    weights = master_new.astype(jnp.bfloat16).reshape(IN, OUT)
    return (master_new, moment_new, second_new, weights)
```

```python
import functools

import jax
import jax.numpy as jnp
from jax import lax
from jax.experimental import pallas as pl
from jax.experimental.pallas import tpu as pltpu
from jax.sharding import PartitionSpec as P

STEP = 1000
MESH = pl.DeviceIdType.MESH
LANE = 128
NX, NY, NZ = 4, 8, 8
ROWS = 24
HALF = 384
AW = 256
CW = 128
F32 = jnp.float32
BF16 = jnp.bfloat16

D0, A1, C1, A2, C2, SS, SO = 0, 2, 5, 12, 19, 22, 29
WS, WO, GA1, GA2, GC1, GC2, DD = 37, 44, 52, 59, 62, 65, 72
NSEM = 84


def kernel(acts, grads, master, moment, second,
           master_out, moment_out, second_out, out,
           acts_v, grads_v, prod, snd0, rcv0, s_a1, r_a1, s_c1, r_c1, s_a2, r_a2, s_c2, r_c2,
           sum3, pack_s, pack_o, s_s, s_o, r_s, r_o, flat, w3s, w3o, s_wo, w24,
           send, recv, local):
    z = lax.axis_index("gx")
    x = lax.axis_index("gy")
    yc = lax.axis_index("gz")
    y = yc // 2
    core = lax.rem(yc, 2)
    other = 1 - core

    def dev(dz=0, dx=0, dy=0, flip=False):
        cc = other if flip else core
        return (lax.rem(z + dz, NZ), lax.rem(x + dx, NX), lax.rem(y + dy, NY) * 2 + cc)

    sends = []

    def push(src, dst, slot, to):
        copy = pltpu.make_async_remote_copy(
            src_ref=src, dst_ref=dst, send_sem=send.at[slot], recv_sem=recv.at[slot],
            device_id=to, device_id_type=MESH)
        copy.start()
        sends.append(copy)
        return copy

    loads = [
        pltpu.make_async_copy(acts.at[:, pl.ds(0, HALF)], acts_v.at[:, pl.ds(0, HALF)], local.at[0]),
        pltpu.make_async_copy(grads, grads_v, local.at[1]),
        pltpu.make_async_copy(acts.at[:, pl.ds(HALF, HALF)], acts_v.at[:, pl.ds(HALF, HALF)], local.at[2]),
    ]
    for load in loads:
        load.start()

    barrier = pltpu.get_barrier_semaphore()
    partners = [dev(flip=True)]
    partners += [dev(dx=k) for k in range(1, NX)]
    partners += [dev(dz=k) for k in range(1, NZ)]
    partners += [dev(dy=k) for k in range(1, NY)]
    partners += [dev(dy=k, flip=True) for k in range(1, NY)]
    for to in partners:
        pl.semaphore_signal(barrier, inc=1, device_id=to, device_id_type=MESH)

    mine = pl.ds(pl.multiple_of(core * HALF, LANE), HALF)
    theirs = pl.ds(pl.multiple_of(other * HALF, LANE), HALF)

    def multiply(m):
        prod[pl.ds(m * HALF, HALF), :] = lax.dot_general(
            acts_v[:, pl.ds(m * HALF, HALF)], grads_v[...], (((0,), (0,)), ((), ())),
            preferred_element_type=F32)
        snd0[pl.ds(16 * m, 16)] = prod[pl.ds(m * HALF, HALF), theirs].astype(BF16).reshape(16, ROWS, HALF)

    loads[0].wait()
    loads[1].wait()
    multiply(0)
    pl.semaphore_wait(barrier, len(partners))
    d0 = [push(snd0.at[pl.ds(0, 16)], rcv0.at[pl.ds(0, 16)], D0, dev(flip=True))]
    loads[2].wait()
    multiply(1)
    d0.append(push(snd0.at[pl.ds(16, 16)], rcv0.at[pl.ds(16, 16)], D0 + 1, dev(flip=True)))

    for m in range(2):
        d0[m].wait_recv()

        def add(i, carry):
            row = pl.ds(pl.multiple_of(i * ROWS, 8), ROWS)
            total = (prod[row, mine] + rcv0[i].astype(F32)).astype(BF16)
            s_a1[lax.rem(i, NX), i // NX] = total[:, :AW]
            s_c1[i // NX, lax.rem(i, NX)] = total[:, AW:]
            return carry

        lax.fori_loop(16 * m, 16 * m + 16, add, 0)

    a1 = [push(s_a1.at[lax.rem(x + k, NX)], r_a1.at[k - 1], A1 + k - 1, dev(dx=k)) for k in (2, 1, 3)]
    c1 = [push(s_c1.at[lax.rem(z + k, NZ)], r_c1.at[k - 1], C1 + k - 1, dev(dz=k)) for k in (4, 3, 5, 2, 6, 1, 7)]

    for copy in c1:
        copy.wait_recv()
    for i in range(NX):
        total = s_c1[z, i].astype(F32)
        for k in range(NZ - 1):
            total += r_c1[k, i].astype(F32)
        s_c2[i] = total.astype(BF16)
    c2 = [push(s_c2.at[lax.rem(x + k, NX)], r_c2.at[k - 1], C2 + k - 1, dev(dx=k)) for k in (2, 1, 3)]

    for copy in a1:
        copy.wait_recv()

    def add_a(i, carry):
        total = s_a1[x, i].astype(F32)
        for k in range(NX - 1):
            total += r_a1[k, i].astype(F32)
        s_a2[i] = total.astype(BF16)
        return carry

    lax.fori_loop(0, NZ, add_a, 0)
    a2 = [push(s_a2.at[lax.rem(z + k, NZ)], r_a2.at[k - 1], A2 + k - 1, dev(dz=k)) for k in (4, 3, 5, 2, 6, 1, 7)]

    for copy in c2:
        copy.wait_recv()
    total = s_c2[x].astype(F32)
    for k in range(NX - 1):
        total += r_c2[k].astype(F32)
    sum3[2] = total
    for copy in a2:
        copy.wait_recv()
    total = s_a2[z].astype(F32)
    for k in range(NZ - 1):
        total += r_a2[k].astype(F32)
    sum3[0] = total[:, :LANE]
    sum3[1] = total[:, LANE:]

    pack_s[...] = jnp.zeros_like(pack_s)
    pack_o[...] = jnp.zeros_like(pack_o)
    for j in range(NY):
        for t in range(3):
            for r in range(2):
                pack_s[j, pl.ds(3 * r + t, 1), :] = sum3[t, pl.ds(3 * j + r + core, 1), :]
            pack_o[j, pl.ds(t, 1), :] = sum3[t, pl.ds(3 * j + 2 - 2 * core, 1), :]
    s_s[...] = pack_s[...].astype(BF16)
    s_o[...] = pack_o[...].astype(BF16)
    st = []
    for k in (4, 3, 5, 2, 6, 1, 7):
        to = lax.rem(y + k, NY)
        st.append(push(s_s.at[to], r_s.at[k - 1], SS + k - 1, dev(dy=k)))
        st.append(push(s_o.at[to], r_o.at[k], SO + k, dev(dy=k, flip=True)))
    st.append(push(s_o.at[y], r_o.at[0], SO, dev(flip=True)))
    for copy in st:
        copy.wait_recv()
    same = s_s[y].astype(F32)
    for k in range(NY - 1):
        same += r_s[k].astype(F32)
    rest = r_o[0].astype(F32)
    for k in range(1, NY):
        rest += r_o[k].astype(F32)
    flat[pl.ds(0, 3), :] = same[0:3]
    flat[pl.ds(3, 3), :] = rest[0:3]
    flat[pl.ds(6, 3), :] = same[3:6]

    gradient = flat[pl.ds(0, 9), :]
    moment_new = 0.9 * moment[...] + 0.1 * gradient
    second_new = 0.95 * second[...] + 0.05 * gradient * gradient
    first_fix = 1.0 - 0.9**STEP
    second_fix = 1.0 - 0.95**STEP
    ratio = moment_new / first_fix / (jnp.sqrt(second_new / second_fix) + 1e-08)
    master_new = master[...] - 0.01 * (ratio + 0.01 * master[...])
    master_out[...] = master_new
    moment_out[...] = moment_new
    second_out[...] = second_new

    pack_s[0, pl.ds(0, 3), :] = master_new[0:3]
    pack_s[0, pl.ds(3, 3), :] = master_new[6:9]
    pack_o[0, pl.ds(0, 3), :] = master_new[3:6]
    w3s[y] = pack_s[0].astype(BF16)
    s_wo[...] = pack_o[0].astype(BF16)
    wt = []
    for k in (4, 3, 5, 2, 6, 1, 7):
        wt.append(push(w3s.at[y], w3s.at[y], WS + k - 1, dev(dy=k)))
        wt.append(push(s_wo, w3o.at[y], WO + k, dev(dy=k, flip=True)))
    wt.append(push(s_wo, w3o.at[y], WO, dev(flip=True)))
    for copy in wt:
        copy.wait_recv()
    pack_s[...] = w3s[...].astype(F32)
    pack_o[...] = w3o[...].astype(F32)
    for j in range(NY):
        for t in range(3):
            for r in range(2):
                w24[t, pl.ds(3 * j + r + core, 1), :] = pack_s[j, pl.ds(3 * r + t, 1), :]
            w24[t, pl.ds(3 * j + 2 - 2 * core, 1), :] = pack_o[j, pl.ds(t, 1), :]
    for t in range(3):
        out[z, x, :, pl.ds(pl.multiple_of(core * HALF + t * LANE, LANE), LANE)] = w24[t].astype(BF16)

    al = pl.ds(pl.multiple_of(core * HALF, LANE), AW)
    cl = pl.ds(pl.multiple_of(core * HALF + AW, LANE), CW)
    block_a = out.at[z, x, :, al]
    block_c = out.at[z, x, :, cl]
    gc1 = [push(block_c, block_c, GC1 + k - 1, dev(dx=k)) for k in (2, 1, 3)]
    ga1 = [push(block_a, block_a, GA1 + k - 1, dev(dz=k)) for k in (4, 3, 5, 2, 6, 1, 7)]
    for copy in gc1:
        copy.wait_recv()
    slab_c = out.at[z, :, :, cl]
    gc2 = [push(slab_c, slab_c, GC2 + k - 1, dev(dz=k)) for k in (4, 3, 5, 2, 6, 1, 7)]
    for copy in ga1:
        copy.wait_recv()
    slab_a = out.at[:, x, :, al]
    ga2 = [push(slab_a, slab_a, GA2 + k - 1, dev(dx=k)) for k in (2, 1, 3)]

    dd = [push(slab_a, slab_a, DD, dev(flip=True)), push(slab_c, slab_c, DD + 1, dev(flip=True))]
    for n, k in enumerate((7, 1, 6, 2, 5, 3, 4)):
        gc2[6 - n].wait_recv()
        slab = out.at[lax.rem(z + NZ - k, NZ), :, :, cl]
        dd.append(push(slab, slab, DD + 2 + n, dev(flip=True)))
    for n, k in enumerate((3, 1, 2)):
        ga2[2 - n].wait_recv()
        slab = out.at[:, lax.rem(x + NX - k, NX), :, al]
        dd.append(push(slab, slab, DD + 9 + n, dev(flip=True)))
    for copy in dd:
        copy.wait_recv()
    for copy in sends:
        copy.wait_send()


def shards(acts, grads_out, master, moment, second):
    vmem = pl.BlockSpec(memory_space=pltpu.VMEM)
    anyw = pl.BlockSpec(memory_space=pl.ANY)
    small = jax.ShapeDtypeStruct(master.shape, F32)
    tokens, width = acts.shape
    master_new, moment_new, second_new, out = pl.pallas_call(
        kernel,
        out_shape=(small, small, small, jax.ShapeDtypeStruct((NZ, NX, ROWS, 2 * HALF), BF16)),
        in_specs=[anyw, anyw, vmem, vmem, vmem],
        out_specs=(vmem, vmem, vmem, vmem),
        scratch_shapes=[
            pltpu.VMEM((tokens, width), BF16),
            pltpu.VMEM((tokens, width), BF16),
            pltpu.VMEM((width, width), F32),
            pltpu.VMEM((NZ * NX, ROWS, HALF), BF16),
            pltpu.VMEM((NZ * NX, ROWS, HALF), BF16),
            pltpu.VMEM((NX, NZ, ROWS, AW), BF16),
            pltpu.VMEM((NX - 1, NZ, ROWS, AW), BF16),
            pltpu.VMEM((NZ, NX, ROWS, CW), BF16),
            pltpu.VMEM((NZ - 1, NX, ROWS, CW), BF16),
            pltpu.VMEM((NZ, ROWS, AW), BF16),
            pltpu.VMEM((NZ - 1, ROWS, AW), BF16),
            pltpu.VMEM((NX, ROWS, CW), BF16),
            pltpu.VMEM((NX - 1, ROWS, CW), BF16),
            pltpu.VMEM((3, ROWS, LANE), F32),
            pltpu.VMEM((NY, 8, LANE), F32),
            pltpu.VMEM((NY, 8, LANE), F32),
            pltpu.VMEM((NY, 8, LANE), BF16),
            pltpu.VMEM((NY, 8, LANE), BF16),
            pltpu.VMEM((NY - 1, 8, LANE), BF16),
            pltpu.VMEM((NY, 8, LANE), BF16),
            pltpu.VMEM((16, LANE), F32),
            pltpu.VMEM((NY, 8, LANE), BF16),
            pltpu.VMEM((NY, 8, LANE), BF16),
            pltpu.VMEM((8, LANE), BF16),
            pltpu.VMEM((3, ROWS, LANE), F32),
            pltpu.SemaphoreType.DMA((NSEM,)),
            pltpu.SemaphoreType.DMA((NSEM,)),
            pltpu.SemaphoreType.DMA((3,)),
        ],
        compiler_params=pltpu.CompilerParams(collective_id=0, has_side_effects=True),
        name="step",
    )(acts, grads_out, master, moment, second)
    return master_new, moment_new, second_new, out.reshape(width, width)


def solution(mesh):
    spec = P(("gx", "gy", "gz"), None)
    return jax.shard_map(
        shards, mesh=mesh, in_specs=(spec,) * 5, out_specs=(spec, spec, spec, P()), check_vma=False)
```
